32 devices in a mesh: region: 2 (over x), feat: 4 (over y, core), row: 4 (over z).
Axes of the slice: x: 2, y: 2, z: 4, core: 2. Of those that a mesh axis runs over, the one named last changes fastest.
Arguments:
- samples: bfloat16 [65536, 128], P(('region', 'row')), may hold values from -6 to 6
- targets: bfloat16 [65536, 64], P(('region', 'row')), may hold values from -6 to 6
- member: int32 [65536], P(('region', 'row')), may hold values 0 or 1
- omega: bfloat16 [128, 4096], P(None, 'feat'), may hold values from -0.5 to 0.5
- phase: float32 [4096], P('feat'), may hold values from -3.140625 to 3.140625
- factors: float32 [8192, 1024], P(('region', 'feat')), may hold values from -0.08 to 5, as said below
- weights_init: float32 [8192, 64], P(('region', 'feat'), 'row'), may hold values from -3 to 3
- duals_init: float32 [8192, 64], P(('region', 'feat'), 'row'), may hold values from -2 to 2
- consensus_init: float32 [4096, 64], P('feat', 'row'), may hold values from -3 to 3
- penalty_init: float32 [2], P('region'), may hold values from 2 to 8
Outputs:
- weights: float32 [8192, 64], P(('region', 'feat'), 'row')
- duals: float32 [8192, 64], P(('region', 'feat'), 'row')
- consensus: float32 [4096, 64], P('feat', 'row')
- penalty: float32 [2, 3], P('region')
The draws below stay inside these ranges and needn't reach their ends.
Inputs may be any that keep to these rules, and one draw needn't show every extreme that they name: factors: each 1024 x 1024 block is lower triangular, its diagonal between 3.5 and 5, its entries below the diagonal drawn independently, symmetric about zero and at most 0.08 in magnitude.
All inputs are finite; a program needn't handle non-finite values. No bound on the sum of `member` on one device may be relied on, other than what follows from the above.
Results may differ from the reference program's by a relative error of at most 0.006.
Values may be sent and summed in bfloat16 or wider, within the bound.
A program may use at most 128 MiB of HBM per device.

```python
import math
import jax
import jax.numpy as jnp
from jax import lax

INPUTS = 128
FEATURES = 4096
OUTPUTS = 64
ITERS = 3
BLOCK = 1024
REGIONS = 2
SAMPLES = 32768
N_FEAT = 4


def draw_samples(key, part):
    first_key, second_key = jax.random.split(jax.random.fold_in(key, 17))
    shape = (REGIONS * SAMPLES, INPUTS)
    values = jax.random.uniform(first_key, shape, jnp.float32, -6.0, 6.0)
    return values.astype(jnp.bfloat16)


def draw_factors(key, part):
    first_key, second_key = jax.random.split(key)
    height = REGIONS * FEATURES
    below = jnp.clip(jax.random.normal(first_key, (height, BLOCK), jnp.float32), -4.0, 4.0) * 0.02
    diagonal = jax.random.uniform(second_key, (height, 1), jnp.float32, 3.5, 5.0)
    inside = jnp.arange(height) % BLOCK
    column = jnp.arange(BLOCK)
    lower = jnp.where(column[None, :] < inside[:, None], below, 0.0)
    return lower + jnp.where(column[None, :] == inside[:, None], diagonal, 0.0)


def set_ends(result, stream_key, least, top_value):
    longest = result.shape.index(max(result.shape))
    spots = []
    for shift in (0, 1):
        where = [jax.random.randint(jax.random.fold_in(stream_key, axis), (), 0, length) for axis, length in enumerate(result.shape)]
        where[longest] = (where[longest] + shift) % result.shape[longest]
        spots.append(tuple(where))
    return result.at[spots[0]].set(least).at[spots[1]].set(top_value)


def shard_levels(stream_key, extent, pieces, low, high):
    level, own = 1.0, jax.random.fold_in(stream_key, 6)
    for dim, shards_of in pieces:
        steps = jnp.exp(jax.random.uniform(jax.random.fold_in(own, dim), (shards_of,), jnp.float32, low / len(pieces), high / len(pieces)))
        level = level * jnp.repeat(steps, extent[dim] // shards_of).reshape([-1 if axis == dim else 1 for axis in range(len(extent))])
    return level


def gaussian(key, extent, spread, limit, pieces=(), held_as=jnp.bfloat16):
    result = jax.random.normal(key, extent, jnp.float32) * spread
    if len(pieces) > 0:
        result = shard_levels(key, extent, pieces, -0.22, 0.18) * result
    return jnp.clip(result, min=-limit, max=limit).astype(held_as)


def setup_inputs(seed: int = 0) -> dict:
    key_list = jax.random.split(jax.random.key(seed), 11)
    samples = draw_samples(jax.random.fold_in(key_list[10], 71), 0)
    targets = gaussian(key_list[1], (REGIONS * SAMPLES, OUTPUTS), 1.0, 6.0, ((0, 8),))
    member = set_ends((jax.random.randint(key_list[2], (REGIONS * SAMPLES,), 0, 8) < 7).astype(jnp.int32), jax.random.fold_in(key_list[2], 1), 0, 1)
    omega = gaussian(key_list[3], (INPUTS, FEATURES), INPUTS ** -0.5, 0.5, ((1, 4),))
    phase = jnp.clip(jax.random.uniform(key_list[4], (FEATURES,), jnp.float32, -3.140625, 3.140625), -3.140625, 3.140625)
    factors = draw_factors(jax.random.fold_in(key_list[10], 71), 0)
    weights_init = gaussian(key_list[6], (REGIONS * FEATURES, OUTPUTS), 0.5, 3.0, ((0, 8), (1, 4)), jnp.float32)
    duals_init = gaussian(key_list[7], (REGIONS * FEATURES, OUTPUTS), 0.3, 2.0, ((0, 8), (1, 4)), jnp.float32)
    consensus_init = gaussian(key_list[8], (FEATURES, OUTPUTS), 0.5, 3.0, ((0, 4), (1, 4)), jnp.float32)
    penalty_init = jnp.clip(jnp.exp(math.log(8.0) - 1.3862944 * jax.random.uniform(key_list[9], (REGIONS,), jnp.float32) ** shard_levels(key_list[9], (REGIONS,), ((0, 2),), -0.2, 0.2)), 2.0, 8.0)
    return {"samples": samples, "targets": targets, "member": member, "omega": omega, "phase": phase, "factors": factors, "weights_init": weights_init, "duals_init": duals_init, "consensus_init": consensus_init, "penalty_init": penalty_init}


def features_of(inputs, omega, phase):
    angle = jnp.dot(inputs.astype(jnp.float32), omega.astype(jnp.float32), preferred_element_type=jnp.float32) + phase
    return (math.sqrt(2.0 / FEATURES) * jnp.cos(angle)).astype(jnp.bfloat16)

def block_solve(factor, right_side):
    forward = lax.linalg.triangular_solve(factor, right_side, left_side=True, lower=True)
    return lax.linalg.triangular_solve(factor, forward, left_side=True, lower=True, transpose_a=True)

def reference(samples, targets, member, omega, phase, factors, weights_init, duals_init, consensus_init, penalty_init):
    inputs = samples.reshape(REGIONS, SAMPLES, INPUTS)
    wanted = targets.reshape(REGIONS, SAMPLES, OUTPUTS)
    chosen = member.reshape(REGIONS, SAMPLES)
    blocks = factors.reshape(REGIONS, N_FEAT, BLOCK, BLOCK)
    weights = weights_init.reshape(REGIONS, FEATURES, OUTPUTS)
    duals = duals_init.reshape(REGIONS, FEATURES, OUTPUTS)
    consensus = consensus_init
    penalty = penalty_init
    offset = 0.01 * FEATURES * OUTPUTS
    history = []
    for iteration in range(ITERS):

        def region_step(items):
            region_in, region_out, region_mask, region_factor, local, dual, scalar = items
            features = features_of(region_in, omega, phase)
            predicted = jnp.dot(features.astype(jnp.float32), local.astype(jnp.bfloat16).astype(jnp.float32), preferred_element_type=jnp.float32)
            residual = (region_mask.astype(jnp.float32)[:, None] * (predicted - region_out.astype(jnp.float32))).astype(jnp.bfloat16)
            gradient = lax.dot_general(features.astype(jnp.float32), residual.astype(jnp.float32), (((0,), (0,)), ((), ())), preferred_element_type=jnp.float32)
            right_side = gradient + scalar * (local - consensus + dual)
            update = jax.vmap(block_solve)(region_factor, right_side.reshape(N_FEAT, BLOCK, OUTPUTS))
            return local - update.reshape(FEATURES, OUTPUTS)
        weights = lax.map(region_step, (inputs, wanted, chosen, blocks, weights, duals, penalty))
        scaled = penalty[:, None, None]
        updated = lax.optimization_barrier(jnp.sum(scaled * (weights + duals), axis=0)) / jnp.sum(penalty)
        duals = duals + weights - updated
        gap = lax.optimization_barrier(jnp.sum(jnp.square(weights - updated), axis=(1, 2)))
        drift = penalty * penalty * jnp.sum(jnp.square(updated - consensus))
        renewed = penalty * jnp.sqrt((gap + offset) / (drift + offset))
        duals = duals * (penalty / renewed)[:, None, None]
        consensus = updated
        penalty = renewed
        history.append(renewed)
    return (weights.reshape(REGIONS * FEATURES, OUTPUTS), duals.reshape(REGIONS * FEATURES, OUTPUTS), consensus, jnp.stack(history, axis=1))
```

```python
import functools
import math

import jax
import jax.numpy as jnp
from jax import lax
from jax.experimental import pallas as pl
from jax.experimental.pallas import tpu as pltpu
from jax.sharding import PartitionSpec as P

ITERS = 3
CORES = 2
PARTS = 2
MESH = pl.DeviceIdType.MESH
INV_TURN = 1.0 / (2.0 * math.pi)
SINE_TERMS = (6.1875, -40.5, 72.5)
SINE_GAIN = 1.0153050682891251
F32 = jnp.float32
BF16 = jnp.bfloat16


def dot(a, b):
    return lax.dot_general(a, b, (((1,), (0,)), ((), ())), preferred_element_type=F32)


def dot_nt(a, b):
    return lax.dot_general(a, b, (((1,), (1,)), ((), ())), preferred_element_type=F32)


def feature_tile(turns):
    rest = turns - jnp.round(turns)
    wave = (0.25 - jnp.abs(rest)).astype(BF16)
    square = wave * wave
    value = jnp.bfloat16(SINE_TERMS[-1])
    for term in SINE_TERMS[-2::-1]:
        value = value * square + jnp.bfloat16(term)
    return wave * value


def normalise(base, factor_ref, dinv_ref, n_ref):
    size = factor_ref.shape[0]
    for start in range(0, size, base):
        rows = factor_ref[start : start + base, :]
        row = lax.broadcasted_iota(jnp.int32, rows.shape, 0) + start
        column = lax.broadcasted_iota(jnp.int32, rows.shape, 1)
        diagonal = jnp.sum(jnp.where(row == column, rows, 0.0), axis=1, keepdims=True)
        n_ref[start : start + base, :] = jnp.where(row > column, rows / diagonal, 0.0).astype(BF16)
        block = factor_ref[start : start + base, start : start + base]
        inner_row = lax.broadcasted_iota(jnp.int32, block.shape, 0)
        inner_column = lax.broadcasted_iota(jnp.int32, block.shape, 1)
        on = jnp.sum(jnp.where(inner_row == inner_column, block, 0.0), axis=0, keepdims=True)
        dinv_ref[:, start : start + base] = 1.0 / on


def invert(base, n_ref, t_ref):
    size = n_ref.shape[0]
    t_ref[...] = jnp.zeros_like(t_ref)
    powers, totals = [], []
    for start in range(0, size, base):
        power = -n_ref[start : start + base, start : start + base].astype(F32)
        powers.append(power)
        totals.append(power)
    reach = 2
    while reach < base:
        for index in range(len(powers)):
            low = powers[index].astype(BF16)
            square = dot(low, low)
            low = square.astype(BF16)
            totals[index] = totals[index] + square + dot(totals[index].astype(BF16), low)
            powers[index] = square
        reach *= 2
    for index, start in enumerate(range(0, size, base)):
        t_ref[start : start + base, start : start + base] = totals[index].astype(BF16)
    width = base
    while width < size:
        for start in range(0, size, 2 * width):
            top = slice(start, start + width)
            bottom = slice(start + width, start + 2 * width)
            below = n_ref[bottom, top]
            first = below.astype(F32) + dot(below, t_ref[top, top])
            second = first + dot(t_ref[bottom, bottom], first.astype(BF16))
            t_ref[bottom, top] = (-second).astype(BF16)
        width *= 2


def admm_kernel(
    sizes,
    offset,
    gain,
    penalty_ref,
    samples_hbm,
    targets_hbm,
    member_hbm,
    omega_ref,
    phase_ref,
    factor_hbm,
    weights_ref,
    duals_ref,
    consensus_ref,
    out_ref,
    history_ref,
    factor_ref,
    dinv_ref,
    strict_ref,
    solve_ref,
    samples_ref,
    targets_ref,
    member_ref,
    far_omega_ref,
    far_phase_ref,
    wave_ref,
    twin_ref,
    feat_ref,
    across_ref,
    coarse_ref,
    acc_ref,
    part_ref,
    other_ref,
    resid_ref,
    total_ref,
    gfar_ref,
    gside_ref,
    gsum_ref,
    gsend_ref,
    grow_ref,
    reg_ref,
    gap_ref,
    load_sem,
    omega_send,
    omega_recv,
    crow_send,
    crow_recv,
    cside_send,
    cside_recv,
    core_send,
    core_recv,
    gside_send,
    gside_recv,
    grow_send,
    grow_recv,
    reg_send,
    reg_recv,
    gap_send,
    gap_recv,
):
    n_region, n_feat, n_row = sizes
    narrow, width = weights_ref.shape
    outputs = n_row * narrow
    count = feat_ref.shape[2]
    chunk = min(1024, count)
    chunks = count // chunk
    piece_width = width // PARTS
    tile = min(512, width)
    inputs = samples_ref.shape[1]
    region, feat, row = lax.axis_index("region"), lax.axis_index("feat"), lax.axis_index("row")
    group = n_feat * n_row
    place = feat * n_row + row
    side = (region, lax.rem(feat + CORES, n_feat), row)
    core = (region, feat + 1 - 2 * lax.rem(feat, CORES), row)

    def row_peer(k):
        return (region, feat, lax.rem(row + k, n_row))

    def region_peer(k):
        return (lax.rem(region + k, n_region), feat, row)

    def group_peer(k):
        other = lax.rem(place + k, group)
        return (region, other // n_row, lax.rem(other, n_row))

    def remote(src, dst, send, recv, device):
        return pltpu.make_async_remote_copy(
            src_ref=src, dst_ref=dst, send_sem=send, recv_sem=recv,
            device_id=device, device_id_type=MESH,
        )

    first = pl.multiple_of((feat // CORES) * count, 128)
    span = pl.ds(first, count)
    loads = [
        pltpu.make_async_copy(samples_hbm.at[span], samples_ref, load_sem.at[0]),
        pltpu.make_async_copy(targets_hbm.at[:, span], targets_ref, load_sem.at[1]),
        pltpu.make_async_copy(member_hbm.at[:, span], member_ref, load_sem.at[2]),
        pltpu.make_async_copy(factor_hbm, factor_ref, load_sem.at[3]),
    ]
    for load in loads:
        load.start()

    barrier = pltpu.get_barrier_semaphore()
    for k in range(1, group):
        pl.semaphore_signal(barrier, inc=1, device_id=group_peer(k), device_id_type=MESH)
    for k in range(1, n_region):
        pl.semaphore_signal(barrier, inc=1, device_id=region_peer(k), device_id_type=MESH)

    def prepare(half, omega, phase):
        exact = omega.astype(F32) * INV_TURN
        high = exact.astype(BF16)
        low = exact - high.astype(F32)
        turn = phase * INV_TURN
        first = turn.astype(BF16).astype(F32)
        level = lax.broadcasted_iota(jnp.int32, low.shape, 0)
        low = jnp.where(level == inputs - 2, first, jnp.where(level == inputs - 1, turn - first, low))
        wave_ref[half, :, :inputs] = high.T
        wave_ref[half, :, inputs:] = low.astype(BF16).T

    def fill(half):
        def step(i, carry):
            down = pl.multiple_of(i * tile, tile)
            value = feature_tile(dot_nt(wave_ref[half, pl.ds(down, tile), :], twin_ref[...]))
            feat_ref[half, pl.ds(down, tile), :] = value
            across_ref[half, :, pl.ds(down, tile)] = value.T
            return carry

        lax.fori_loop(0, width // tile, step, 0)

    weights, duals, consensus = weights_ref[...], duals_ref[...], consensus_ref[...]
    rho = jnp.full((1, 128), penalty_ref[0], F32)
    history = jnp.zeros((1, 128), F32)
    lane = lax.broadcasted_iota(jnp.int32, (1, 128), 1)
    prepare(0, omega_ref[...], phase_ref[...])
    loads[0].wait()
    samples = samples_ref[...]
    place_in = lax.broadcasted_iota(jnp.int32, samples.shape, 1)
    twin_ref[:, :inputs] = samples
    twin_ref[:, inputs:] = jnp.where(place_in < inputs - 2, samples.astype(F32), 1.0).astype(BF16)
    pl.semaphore_wait(barrier, group - 1 + n_region - 1)
    sends = []
    exchange = [
        remote(omega_ref, far_omega_ref, omega_send.at[0], omega_recv.at[0], side),
        remote(phase_ref, far_phase_ref, omega_send.at[1], omega_recv.at[1], side),
    ]
    for copy in exchange:
        copy.start()
        sends.append(copy)

    for t in range(ITERS):
        coarse_ref[t, 0, row] = weights.astype(BF16)
        mine = coarse_ref.at[t, 0, row]
        for k in range(1, n_row):
            copy = remote(mine, mine, crow_send.at[t, k], crow_recv.at[t, k], row_peer(k))
            copy.start()
            sends.append(copy)
        copy = remote(
            mine, coarse_ref.at[t, 1, row], cside_send.at[t, 0], cside_recv.at[t, 0], side
        )
        copy.start()
        sends.append(copy)
        if t == 0:
            fill(0)

        for k in range(1, n_row):
            source = lax.rem(row - k + n_row, n_row)
            piece = coarse_ref.at[t, 0, source]
            remote(piece, piece, crow_send.at[t, k], crow_recv.at[t, k], side).wait_recv()
            copy = remote(
                piece, coarse_ref.at[t, 1, source], cside_send.at[t, k], cside_recv.at[t, k], side
            )
            copy.start()
            sends.append(copy)
        near = coarse_ref[t, 0].reshape(outputs, width)
        for j in range(chunks):
            span = slice(j * chunk, (j + 1) * chunk)
            acc_ref[:, span] = dot(near, feat_ref[0, :, span])
        if t > 0:
            duals, consensus = finish_region(t - 1)
        else:
            for copy in exchange:
                copy.wait_recv()
            prepare(1, far_omega_ref[...], far_phase_ref[...])
            fill(1)
            loads[1].wait()
            loads[2].wait()
        for k in range(n_row):
            source = lax.rem(row - k + n_row, n_row)
            piece = coarse_ref.at[t, 1, source]
            remote(piece, piece, cside_send.at[t, k], cside_recv.at[t, k], side).wait_recv()
        far = coarse_ref[t, 1].reshape(outputs, width)
        for j in range(chunks):
            span = slice(j * chunk, (j + 1) * chunk)
            part = acc_ref[:, span] + dot(far, feat_ref[1, :, span])
            acc_ref[:, span] = part
            part_ref[t, j] = part.astype(BF16)
            copy = remote(
                part_ref.at[t, j], other_ref.at[t, j], core_send.at[t, j], core_recv.at[t, j], core
            )
            copy.start()
            sends.append(copy)
        for j in range(chunks):
            span = slice(j * chunk, (j + 1) * chunk)
            piece = other_ref.at[t, j]
            remote(piece, piece, core_send.at[t, j], core_recv.at[t, j], core).wait_recv()
            predicted = gain * (acc_ref[:, span] + other_ref[t, j].astype(F32))
            gap_value = predicted - targets_ref[:, span].astype(F32)
            resid_ref[:, span] = (member_ref[:, span].astype(F32) * gap_value).astype(BF16)
            if j < chunks - 1:
                value = dot(resid_ref[:, span], across_ref[1, span, :])
                total_ref[...] = value if j == 0 else total_ref[...] + value

        last = slice((chunks - 1) * chunk, chunks * chunk)
        for p in range(PARTS):
            span = slice(p * piece_width, (p + 1) * piece_width)
            value = dot(resid_ref[:, last], across_ref[1, last, span])
            if chunks > 1:
                value = value + total_ref[:, span]
            gfar_ref[t, p] = value.astype(BF16).reshape(n_row, narrow, piece_width)
            copy = remote(
                gfar_ref.at[t, p], gside_ref.at[t, p], gside_send.at[t, p], gside_recv.at[t, p],
                side,
            )
            copy.start()
            sends.append(copy)
        for p in range(PARTS):
            span = slice(p * piece_width, (p + 1) * piece_width)
            value = dot(resid_ref[...], across_ref[0, :, span])
            gsum_ref[p] = value.reshape(n_row, narrow, piece_width)
        if t == 0:
            loads[3].wait()
            normalise(min(256, width), factor_ref, dinv_ref, strict_ref)
        for p in range(PARTS):
            piece = gside_ref.at[t, p]
            remote(piece, piece, gside_send.at[t, p], gside_recv.at[t, p], side).wait_recv()
            for k in range(1, n_row):
                target = lax.rem(row + k, n_row)
                value = gsum_ref[p, target] + gside_ref[t, p, target].astype(F32)
                gsend_ref[t, p, k] = value.astype(BF16)
                copy = remote(
                    gsend_ref.at[t, p, k], grow_ref.at[t, p, k], grow_send.at[t, p, k],
                    grow_recv.at[t, p, k], row_peer(k),
                )
                copy.start()
                sends.append(copy)
        if t > 0:
            rho, duals, history = finish_gap(t - 1, rho, duals, history)
        else:
            invert(min(256, width), strict_ref, solve_ref)
        dinv = dinv_ref[...]
        scalar = rho[:, :1]
        gradient = []
        for p in range(PARTS):
            value = gsum_ref[p, row] + gside_ref[t, p, row].astype(F32)
            for k in range(1, n_row):
                piece = grow_ref.at[t, p, k]
                remote(
                    piece, piece, grow_send.at[t, p, k], grow_recv.at[t, p, k], side
                ).wait_recv()
                value = value + grow_ref[t, p, k].astype(F32)
            gradient.append(value)
        right = scalar * (weights - consensus + duals) + gain * jnp.concatenate(gradient, axis=1)
        forward = right * dinv
        forward = forward + dot_nt(forward.astype(BF16), solve_ref[...])
        backward = (forward + dot(forward.astype(BF16), solve_ref[...])) * dinv
        weights = weights - backward

        reg_ref[t, region, :narrow] = scalar * (weights + duals)
        reg_ref[t, region, narrow:] = jnp.broadcast_to(scalar, (8, width))
        mine = reg_ref.at[t, region]
        for k in range(1, n_region):
            copy = remote(mine, mine, reg_send.at[t, k], reg_recv.at[t, k], region_peer(k))
            copy.start()
            sends.append(copy)

        def finish_region(s, weights=weights, duals=duals, consensus=consensus):
            for k in range(1, n_region):
                source = lax.rem(region - k + n_region, n_region)
                piece = reg_ref.at[s, source]
                remote(
                    piece, piece, reg_send.at[s, k], reg_recv.at[s, k], region_peer(k)
                ).wait_recv()
            total = reg_ref[s, 0]
            for r in range(1, n_region):
                total = total + reg_ref[s, r]
            updated = total[:narrow] / total[narrow : narrow + 1]
            gap = jnp.sum(jnp.square(weights - updated), keepdims=True).reshape(1, 1)
            drift = jnp.sum(jnp.square(updated - consensus), keepdims=True).reshape(1, 1)
            level = lax.broadcasted_iota(jnp.int32, (8, 128), 0)
            gap_ref[s, place] = jnp.where(level == 0, gap, drift)
            mine = gap_ref.at[s, place]
            for k in range(1, group):
                copy = remote(mine, mine, gap_send.at[s, k], gap_recv.at[s, k], group_peer(k))
                copy.start()
                sends.append(copy)
            return duals + weights - updated, updated

        def finish_gap(s, rho, duals, history):
            for k in range(1, group):
                source = lax.rem(place - k + group, group)
                piece = gap_ref.at[s, source]
                remote(
                    piece, piece, gap_send.at[s, k], gap_recv.at[s, k], group_peer(k)
                ).wait_recv()
            total = jnp.sum(gap_ref[s], axis=0)
            gap, drift = total[0:1], total[1:2]
            drift = rho * rho * drift
            renewed = rho * jnp.sqrt((gap + offset) / (drift + offset))
            duals = duals * (rho / renewed)[:, :1]
            return renewed, duals, jnp.where(lane == s, renewed, history)

    duals, consensus = finish_region(ITERS - 1)
    rho, duals, history = finish_gap(ITERS - 1, rho, duals, history)
    out_ref[0] = weights
    out_ref[1] = duals
    out_ref[2] = consensus
    history_ref[...] = history
    for copy in sends:
        copy.wait_send()


def admm(sizes, offset, gain, penalty, samples, targets, member, omega, phase, factors, *state):
    n_region, n_feat, n_row = sizes
    narrow, width = state[0].shape
    outputs = n_row * narrow
    inputs = omega.shape[0]
    count = samples.shape[0] // (n_feat // CORES)
    chunk = min(1024, count)
    chunks = count // chunk
    group = n_feat * n_row
    part = (n_row, narrow, width // PARTS)
    vmem = pl.BlockSpec(memory_space=pltpu.VMEM)
    hbm = pl.BlockSpec(memory_space=pl.ANY)
    dma = pltpu.SemaphoreType.DMA
    return pl.pallas_call(
        functools.partial(admm_kernel, sizes, offset, gain),
        in_specs=[pl.BlockSpec(memory_space=pltpu.SMEM), hbm, hbm, hbm] + [vmem, vmem, hbm, vmem, vmem, vmem],
        out_specs=[vmem, vmem],
        out_shape=[
            jax.ShapeDtypeStruct((3, narrow, width), F32),
            jax.ShapeDtypeStruct((1, 128), F32),
        ],
        scratch_shapes=[
            pltpu.VMEM((width, width), F32),
            pltpu.VMEM((1, width), F32),
            pltpu.VMEM((width, width), BF16),
            pltpu.VMEM((width, width), BF16),
            pltpu.VMEM((count, inputs), BF16),
            pltpu.VMEM((outputs, count), BF16),
            pltpu.VMEM((1, count), jnp.int32),
            pltpu.VMEM((inputs, width), BF16),
            pltpu.VMEM((1, width), F32),
            pltpu.VMEM((2, width, 2 * inputs), BF16),
            pltpu.VMEM((count, 2 * inputs), BF16),
            pltpu.VMEM((2, width, count), BF16),
            pltpu.VMEM((2, count, width), BF16),
            pltpu.VMEM((ITERS, 2, n_row, narrow, width), BF16),
            pltpu.VMEM((outputs, count), F32),
            pltpu.VMEM((ITERS, chunks, outputs, chunk), BF16),
            pltpu.VMEM((ITERS, chunks, outputs, chunk), BF16),
            pltpu.VMEM((outputs, count), BF16),
            pltpu.VMEM((outputs, width), F32),
            pltpu.VMEM((ITERS, PARTS) + part, BF16),
            pltpu.VMEM((ITERS, PARTS) + part, BF16),
            pltpu.VMEM((PARTS,) + part, F32),
            pltpu.VMEM((ITERS, PARTS) + part, BF16),
            pltpu.VMEM((ITERS, PARTS) + part, BF16),
            pltpu.VMEM((ITERS, n_region, narrow + 8, width), F32),
            pltpu.VMEM((ITERS, group, 8, 128), F32),
            dma((4,)),
            dma((2,)),
            dma((2,)),
            dma((ITERS, n_row)),
            dma((ITERS, n_row)),
            dma((ITERS, n_row)),
            dma((ITERS, n_row)),
            dma((ITERS, chunks)),
            dma((ITERS, chunks)),
            dma((ITERS, PARTS)),
            dma((ITERS, PARTS)),
            dma((ITERS, PARTS, n_row)),
            dma((ITERS, PARTS, n_row)),
            dma((ITERS, n_region)),
            dma((ITERS, n_region)),
            dma((ITERS, group)),
            dma((ITERS, group)),
        ],
        compiler_params=pltpu.CompilerParams(
            collective_id=0, has_side_effects=True, vmem_limit_bytes=60 * 2**20
        ),
        name="admm",
    )(penalty, samples, targets, member, omega, phase, factors, *state)


def per_device(
    sizes,
    samples,
    targets,
    member,
    omega,
    phase,
    factors,
    weights_init,
    duals_init,
    consensus_init,
    penalty_init,
):
    n_region, n_feat, n_row = sizes
    total_features = n_feat * omega.shape[1]
    total_outputs = targets.shape[1]
    offset = 0.01 * total_features * total_outputs
    gain = SINE_GAIN * math.sqrt(2.0 / total_features)
    final, history = admm(
        sizes, offset, gain, penalty_init, samples, targets.T, member[None, :], omega,
        phase[None, :], factors, weights_init.T, duals_init.T, consensus_init.T,
    )
    return (final[0].T, final[1].T, final[2].T, history[:, :ITERS])


def solution(mesh):
    sizes = (mesh.shape["region"], mesh.shape["feat"], mesh.shape["row"])
    return jax.shard_map(
        functools.partial(per_device, sizes),
        mesh=mesh,
        in_specs=(
            P(("region", "row"), None),
            P(("region", "row"), None),
            P(("region", "row")),
            P(None, "feat"),
            P("feat"),
            P(("region", "feat"), None),
            P(("region", "feat"), "row"),
            P(("region", "feat"), "row"),
            P("feat", "row"),
            P("region"),
        ),
        out_specs=(
            P(("region", "feat"), "row"),
            P(("region", "feat"), "row"),
            P("feat", "row"),
            P("region", None),
        ),
        check_vma=False,
    )
```

```python
import functools
import math

import jax
import jax.numpy as jnp
from jax import lax
from jax.experimental import pallas as pl
from jax.experimental.pallas import tpu as pltpu
from jax.sharding import PartitionSpec as P

ITERS = 3
CORES = 2
PARTS = 2
MESH = pl.DeviceIdType.MESH
INV_TURN = 1.0 / (2.0 * math.pi)
SINE_TERMS = (6.1875, -40.5, 72.5)
SINE_GAIN = 1.0153050682891251
F32 = jnp.float32
BF16 = jnp.bfloat16


def dot(a, b):
    return lax.dot_general(a, b, (((1,), (0,)), ((), ())), preferred_element_type=F32)


def dot_nt(a, b):
    return lax.dot_general(a, b, (((1,), (1,)), ((), ())), preferred_element_type=F32)


def feature_tile(turns):
    rest = turns - jnp.round(turns)
    wave = (0.25 - jnp.abs(rest)).astype(BF16)
    square = wave * wave
    value = jnp.bfloat16(SINE_TERMS[-1])
    for term in SINE_TERMS[-2::-1]:
        value = value * square + jnp.bfloat16(term)
    return wave * value


def normalise(base, factor_ref, dinv_ref, n_ref):
    size = factor_ref.shape[0]
    for start in range(0, size, base):
        rows = factor_ref[start : start + base, :]
        row = lax.broadcasted_iota(jnp.int32, rows.shape, 0) + start
        column = lax.broadcasted_iota(jnp.int32, rows.shape, 1)
        diagonal = jnp.sum(jnp.where(row == column, rows, 0.0), axis=1, keepdims=True)
        n_ref[start : start + base, :] = jnp.where(row > column, rows / diagonal, 0.0).astype(BF16)
        block = factor_ref[start : start + base, start : start + base]
        inner_row = lax.broadcasted_iota(jnp.int32, block.shape, 0)
        inner_column = lax.broadcasted_iota(jnp.int32, block.shape, 1)
        on = jnp.sum(jnp.where(inner_row == inner_column, block, 0.0), axis=0, keepdims=True)
        dinv_ref[:, start : start + base] = 1.0 / on


def invert(base, n_ref, t_ref):
    size = n_ref.shape[0]
    t_ref[...] = jnp.zeros_like(t_ref)
    powers, totals = [], []
    for start in range(0, size, base):
        power = -n_ref[start : start + base, start : start + base].astype(F32)
        powers.append(power)
        totals.append(power)
    reach = 2
    while reach < base:
        for index in range(len(powers)):
            low = powers[index].astype(BF16)
            square = dot(low, low)
            low = square.astype(BF16)
            totals[index] = totals[index] + square + dot(totals[index].astype(BF16), low)
            powers[index] = square
        reach *= 2
    for index, start in enumerate(range(0, size, base)):
        t_ref[start : start + base, start : start + base] = totals[index].astype(BF16)
    width = base
    while width < size:
        for start in range(0, size, 2 * width):
            top = slice(start, start + width)
            bottom = slice(start + width, start + 2 * width)
            below = n_ref[bottom, top]
            first = below.astype(F32) + dot(below, t_ref[top, top])
            second = first + dot(t_ref[bottom, bottom], first.astype(BF16))
            t_ref[bottom, top] = (-second).astype(BF16)
        width *= 2


def admm_kernel(
    sizes,
    offset,
    gain,
    penalty_ref,
    samples_hbm,
    targets_hbm,
    member_hbm,
    omega_hbm,
    phase_hbm,
    factor_hbm,
    weights_hbm,
    duals_hbm,
    consensus_hbm,
    out_ref,
    history_ref,
    omega_ref,
    phase_ref,
    state_ref,
    factor_ref,
    dinv_ref,
    strict_ref,
    solve_ref,
    samples_ref,
    targets_ref,
    member_ref,
    far_omega_ref,
    far_phase_ref,
    wave_ref,
    twin_ref,
    feat_ref,
    across_ref,
    coarse_ref,
    acc_ref,
    part_ref,
    other_ref,
    resid_ref,
    total_ref,
    gfar_ref,
    gside_ref,
    gsum_ref,
    gsend_ref,
    grow_ref,
    reg_ref,
    gap_ref,
    load_sem,
    omega_send,
    omega_recv,
    crow_send,
    crow_recv,
    cside_send,
    cside_recv,
    core_send,
    core_recv,
    gside_send,
    gside_recv,
    grow_send,
    grow_recv,
    reg_send,
    reg_recv,
    gap_send,
    gap_recv,
):
    n_region, n_feat, n_row = sizes
    narrow, width = weights_hbm.shape
    outputs = n_row * narrow
    count = feat_ref.shape[2]
    chunk = min(1024, count)
    chunks = count // chunk
    piece_width = width // PARTS
    tile = min(512, width)
    inputs = samples_ref.shape[1]
    region, feat, row = lax.axis_index("region"), lax.axis_index("feat"), lax.axis_index("row")
    outward = sorted(range(1, n_row), key=lambda k: -min(k, n_row - k))
    inward = outward[::-1]
    group = n_feat * n_row
    place = feat * n_row + row
    across_feat = lax.rem(feat + CORES, n_feat)
    side = (region, across_feat + 1 - 2 * lax.rem(across_feat, CORES), row)
    core = (region, feat + 1 - 2 * lax.rem(feat, CORES), row)

    def row_peer(k):
        return (region, feat, lax.rem(row + k, n_row))

    def region_peer(k):
        return (lax.rem(region + k, n_region), feat, row)

    def group_peer(k):
        other = lax.rem(place + k, group)
        return (region, other // n_row, lax.rem(other, n_row))

    def remote(src, dst, send, recv, device):
        return pltpu.make_async_remote_copy(
            src_ref=src, dst_ref=dst, send_sem=send, recv_sem=recv,
            device_id=device, device_id_type=MESH,
        )

    first = pl.multiple_of((feat // CORES) * count, 128)
    span = pl.ds(first, count)
    loads = [
        pltpu.make_async_copy(samples_hbm.at[span], samples_ref, load_sem.at[0]),
        pltpu.make_async_copy(targets_hbm.at[:, span], targets_ref, load_sem.at[1]),
        pltpu.make_async_copy(member_hbm.at[:, span], member_ref, load_sem.at[2]),
        pltpu.make_async_copy(factor_hbm, factor_ref, load_sem.at[3]),
        pltpu.make_async_copy(omega_hbm, omega_ref, load_sem.at[4]),
        pltpu.make_async_copy(phase_hbm, phase_ref, load_sem.at[5]),
        pltpu.make_async_copy(weights_hbm, state_ref.at[0], load_sem.at[6]),
        pltpu.make_async_copy(duals_hbm, state_ref.at[1], load_sem.at[7]),
        pltpu.make_async_copy(consensus_hbm, state_ref.at[2], load_sem.at[8]),
    ]
    for index in (4, 5, 0, 6, 7, 8, 1, 2, 3):
        loads[index].start()

    barrier = pltpu.get_barrier_semaphore()
    for k in range(1, group):
        pl.semaphore_signal(barrier, inc=1, device_id=group_peer(k), device_id_type=MESH)
    for k in range(1, n_region):
        pl.semaphore_signal(barrier, inc=1, device_id=region_peer(k), device_id_type=MESH)

    def prepare(half, omega, phase):
        exact = omega.astype(F32) * INV_TURN
        high = exact.astype(BF16)
        low = exact - high.astype(F32)
        turn = phase * INV_TURN
        first = turn.astype(BF16).astype(F32)
        level = lax.broadcasted_iota(jnp.int32, low.shape, 0)
        low = jnp.where(level == inputs - 2, first, jnp.where(level == inputs - 1, turn - first, low))
        wave_ref[half, :, :inputs] = high.T
        wave_ref[half, :, inputs:] = low.astype(BF16).T

    def fill(half):
        def step(i, carry):
            down = pl.multiple_of(i * tile, tile)
            value = feature_tile(dot_nt(wave_ref[half, pl.ds(down, tile), :], twin_ref[...]))
            feat_ref[half, pl.ds(down, tile), :] = value
            across_ref[half, :, pl.ds(down, tile)] = value.T
            return carry

        lax.fori_loop(0, width // tile, step, 0)

    rho = jnp.full((1, 128), penalty_ref[0], F32)
    history = jnp.zeros((1, 128), F32)
    lane = lax.broadcasted_iota(jnp.int32, (1, 128), 1)
    loads[4].wait()
    loads[5].wait()
    prepare(0, omega_ref[...], phase_ref[...])
    loads[0].wait()
    samples = samples_ref[...]
    place_in = lax.broadcasted_iota(jnp.int32, samples.shape, 1)
    twin_ref[:, :inputs] = samples
    twin_ref[:, inputs:] = jnp.where(place_in < inputs - 2, samples.astype(F32), 1.0).astype(BF16)
    for index in (6, 7, 8):
        loads[index].wait()
    weights, duals, consensus = state_ref[0], state_ref[1], state_ref[2]
    pl.semaphore_wait(barrier, group - 1 + n_region - 1)
    sends = []
    exchange = [
        remote(omega_ref, far_omega_ref, omega_send.at[0], omega_recv.at[0], side),
        remote(phase_ref, far_phase_ref, omega_send.at[1], omega_recv.at[1], side),
    ]
    for copy in exchange:
        copy.start()
        sends.append(copy)

    for t in range(ITERS):
        coarse_ref[t, 0, row] = weights.astype(BF16)
        mine = coarse_ref.at[t, 0, row]
        for k in outward:
            copy = remote(mine, mine, crow_send.at[t, k], crow_recv.at[t, k], row_peer(k))
            copy.start()
            sends.append(copy)
        copy = remote(
            mine, coarse_ref.at[t, 1, row], cside_send.at[t, 0], cside_recv.at[t, 0], side
        )
        copy.start()
        sends.append(copy)
        if t == 0:
            fill(0)

        for k in inward:
            source = lax.rem(row - k + n_row, n_row)
            piece = coarse_ref.at[t, 0, source]
            remote(piece, piece, crow_send.at[t, k], crow_recv.at[t, k], side).wait_recv()
            copy = remote(
                piece, coarse_ref.at[t, 1, source], cside_send.at[t, k], cside_recv.at[t, k], side
            )
            copy.start()
            sends.append(copy)
        near = coarse_ref[t, 0].reshape(outputs, width)
        for j in range(chunks):
            span = slice(j * chunk, (j + 1) * chunk)
            acc_ref[:, span] = dot(near, feat_ref[0, :, span])
        if t > 0:
            duals, consensus = finish_region(t - 1)
        else:
            for copy in exchange:
                copy.wait_recv()
            prepare(1, far_omega_ref[...], far_phase_ref[...])
            fill(1)
            loads[1].wait()
            loads[2].wait()
        for k in range(n_row):
            source = lax.rem(row - k + n_row, n_row)
            piece = coarse_ref.at[t, 1, source]
            remote(piece, piece, cside_send.at[t, k], cside_recv.at[t, k], side).wait_recv()
        far = coarse_ref[t, 1].reshape(outputs, width)
        for j in range(chunks):
            span = slice(j * chunk, (j + 1) * chunk)
            part = acc_ref[:, span] + dot(far, feat_ref[1, :, span])
            acc_ref[:, span] = part
            part_ref[t, j] = part.astype(BF16)
            copy = remote(
                part_ref.at[t, j], other_ref.at[t, j], core_send.at[t, j], core_recv.at[t, j], core
            )
            copy.start()
            sends.append(copy)
        for j in range(chunks):
            span = slice(j * chunk, (j + 1) * chunk)
            piece = other_ref.at[t, j]
            remote(piece, piece, core_send.at[t, j], core_recv.at[t, j], core).wait_recv()
            predicted = gain * (acc_ref[:, span] + other_ref[t, j].astype(F32))
            gap_value = predicted - targets_ref[:, span].astype(F32)
            resid_ref[:, span] = (member_ref[:, span].astype(F32) * gap_value).astype(BF16)
            if j < chunks - 1:
                value = dot(resid_ref[:, span], across_ref[1, span, :])
                total_ref[...] = value if j == 0 else total_ref[...] + value

        last = slice((chunks - 1) * chunk, chunks * chunk)
        for p in range(PARTS):
            span = slice(p * piece_width, (p + 1) * piece_width)
            value = dot(resid_ref[:, last], across_ref[1, last, span])
            if chunks > 1:
                value = value + total_ref[:, span]
            gfar_ref[t, p] = value.astype(BF16).reshape(n_row, narrow, piece_width)
            copy = remote(
                gfar_ref.at[t, p], gside_ref.at[t, p], gside_send.at[t, p], gside_recv.at[t, p],
                side,
            )
            copy.start()
            sends.append(copy)
        for p in range(PARTS):
            span = slice(p * piece_width, (p + 1) * piece_width)
            value = dot(resid_ref[...], across_ref[0, :, span])
            gsum_ref[p] = value.reshape(n_row, narrow, piece_width)
        if t == 0:
            loads[3].wait()
            normalise(min(256, width), factor_ref, dinv_ref, strict_ref)
        for p in range(PARTS):
            piece = gside_ref.at[t, p]
            remote(piece, piece, gside_send.at[t, p], gside_recv.at[t, p], side).wait_recv()
            for k in outward:
                target = lax.rem(row + k, n_row)
                value = gsum_ref[p, target] + gside_ref[t, p, target].astype(F32)
                gsend_ref[t, p, k] = value.astype(BF16)
                copy = remote(
                    gsend_ref.at[t, p, k], grow_ref.at[t, p, k], grow_send.at[t, p, k],
                    grow_recv.at[t, p, k], row_peer(k),
                )
                copy.start()
                sends.append(copy)
        if t > 0:
            rho, duals, history = finish_gap(t - 1, rho, duals, history)
        else:
            invert(min(256, width), strict_ref, solve_ref)
        dinv = dinv_ref[...]
        scalar = rho[:, :1]
        gradient = []
        for p in range(PARTS):
            value = gsum_ref[p, row] + gside_ref[t, p, row].astype(F32)
            for k in range(1, n_row):
                piece = grow_ref.at[t, p, k]
                remote(
                    piece, piece, grow_send.at[t, p, k], grow_recv.at[t, p, k], side
                ).wait_recv()
                value = value + grow_ref[t, p, k].astype(F32)
            gradient.append(value)
        right = scalar * (weights - consensus + duals) + gain * jnp.concatenate(gradient, axis=1)
        forward = right * dinv
        forward = forward + dot_nt(forward.astype(BF16), solve_ref[...])
        backward = (forward + dot(forward.astype(BF16), solve_ref[...])) * dinv
        weights = weights - backward

        reg_ref[t, region, :narrow] = scalar * (weights + duals)
        reg_ref[t, region, narrow:] = jnp.broadcast_to(scalar, (8, width))
        mine = reg_ref.at[t, region]
        for k in range(1, n_region):
            copy = remote(mine, mine, reg_send.at[t, k], reg_recv.at[t, k], region_peer(k))
            copy.start()
            sends.append(copy)

        def finish_region(s, weights=weights, duals=duals, consensus=consensus):
            for k in range(1, n_region):
                source = lax.rem(region - k + n_region, n_region)
                piece = reg_ref.at[s, source]
                remote(
                    piece, piece, reg_send.at[s, k], reg_recv.at[s, k], region_peer(k)
                ).wait_recv()
            total = reg_ref[s, 0]
            for r in range(1, n_region):
                total = total + reg_ref[s, r]
            updated = total[:narrow] / total[narrow : narrow + 1]
            gap = jnp.sum(jnp.square(weights - updated), keepdims=True).reshape(1, 1)
            drift = jnp.sum(jnp.square(updated - consensus), keepdims=True).reshape(1, 1)
            level = lax.broadcasted_iota(jnp.int32, (8, 128), 0)
            gap_ref[s, place] = jnp.where(level == 0, gap, drift)
            mine = gap_ref.at[s, place]
            for k in range(1, group):
                copy = remote(mine, mine, gap_send.at[s, k], gap_recv.at[s, k], group_peer(k))
                copy.start()
                sends.append(copy)
            return duals + weights - updated, updated

        def finish_gap(s, rho, duals, history):
            for k in range(1, group):
                source = lax.rem(place - k + group, group)
                piece = gap_ref.at[s, source]
                remote(
                    piece, piece, gap_send.at[s, k], gap_recv.at[s, k], group_peer(k)
                ).wait_recv()
            total = jnp.sum(gap_ref[s], axis=0)
            gap, drift = total[0:1], total[1:2]
            drift = rho * rho * drift
            renewed = rho * jnp.sqrt((gap + offset) / (drift + offset))
            duals = duals * (rho / renewed)[:, :1]
            return renewed, duals, jnp.where(lane == s, renewed, history)

    duals, consensus = finish_region(ITERS - 1)
    rho, duals, history = finish_gap(ITERS - 1, rho, duals, history)
    out_ref[0] = weights
    out_ref[1] = duals
    out_ref[2] = consensus
    history_ref[...] = history
    for copy in sends:
        copy.wait_send()


def admm(sizes, offset, gain, penalty, samples, targets, member, omega, phase, factors, *state):
    n_region, n_feat, n_row = sizes
    narrow, width = state[0].shape
    outputs = n_row * narrow
    inputs = omega.shape[0]
    count = samples.shape[0] // (n_feat // CORES)
    chunk = min(1024, count)
    chunks = count // chunk
    group = n_feat * n_row
    part = (n_row, narrow, width // PARTS)
    vmem = pl.BlockSpec(memory_space=pltpu.VMEM)
    hbm = pl.BlockSpec(memory_space=pl.ANY)
    dma = pltpu.SemaphoreType.DMA
    return pl.pallas_call(
        functools.partial(admm_kernel, sizes, offset, gain),
        in_specs=[pl.BlockSpec(memory_space=pltpu.SMEM), ] + [hbm] * 9,
        out_specs=[vmem, vmem],
        out_shape=[
            pltpu.VMEM((3, narrow, width), F32),
            pltpu.VMEM((1, 128), F32),
        ],
        scratch_shapes=[
            pltpu.VMEM((inputs, width), BF16),
            pltpu.VMEM((1, width), F32),
            pltpu.VMEM((3, narrow, width), F32),
            pltpu.VMEM((width, width), F32),
            pltpu.VMEM((1, width), F32),
            pltpu.VMEM((width, width), BF16),
            pltpu.VMEM((width, width), BF16),
            pltpu.VMEM((count, inputs), BF16),
            pltpu.VMEM((outputs, count), BF16),
            pltpu.VMEM((1, count), jnp.int32),
            pltpu.VMEM((inputs, width), BF16),
            pltpu.VMEM((1, width), F32),
            pltpu.VMEM((2, width, 2 * inputs), BF16),
            pltpu.VMEM((count, 2 * inputs), BF16),
            pltpu.VMEM((2, width, count), BF16),
            pltpu.VMEM((2, count, width), BF16),
            pltpu.VMEM((ITERS, 2, n_row, narrow, width), BF16),
            pltpu.VMEM((outputs, count), F32),
            pltpu.VMEM((ITERS, chunks, outputs, chunk), BF16),
            pltpu.VMEM((ITERS, chunks, outputs, chunk), BF16),
            pltpu.VMEM((outputs, count), BF16),
            pltpu.VMEM((outputs, width), F32),
            pltpu.VMEM((ITERS, PARTS) + part, BF16),
            pltpu.VMEM((ITERS, PARTS) + part, BF16),
            pltpu.VMEM((PARTS,) + part, F32),
            pltpu.VMEM((ITERS, PARTS) + part, BF16),
            pltpu.VMEM((ITERS, PARTS) + part, BF16),
            pltpu.VMEM((ITERS, n_region, narrow + 8, width), F32),
            pltpu.VMEM((ITERS, group, 8, 128), F32),
            dma((9,)),
            dma((2,)),
            dma((2,)),
            dma((ITERS, n_row)),
            dma((ITERS, n_row)),
            dma((ITERS, n_row)),
            dma((ITERS, n_row)),
            dma((ITERS, chunks)),
            dma((ITERS, chunks)),
            dma((ITERS, PARTS)),
            dma((ITERS, PARTS)),
            dma((ITERS, PARTS, n_row)),
            dma((ITERS, PARTS, n_row)),
            dma((ITERS, n_region)),
            dma((ITERS, n_region)),
            dma((ITERS, group)),
            dma((ITERS, group)),
        ],
        compiler_params=pltpu.CompilerParams(
            collective_id=0, has_side_effects=True, vmem_limit_bytes=60 * 2**20
        ),
        name="admm",
    )(penalty, samples, targets, member, omega, phase, factors, *state)


def per_device(
    sizes,
    samples,
    targets,
    member,
    omega,
    phase,
    factors,
    weights_init,
    duals_init,
    consensus_init,
    penalty_init,
):
    n_region, n_feat, n_row = sizes
    total_features = n_feat * omega.shape[1]
    total_outputs = targets.shape[1]
    offset = 0.01 * total_features * total_outputs
    gain = SINE_GAIN * math.sqrt(2.0 / total_features)
    final, history = admm(
        sizes, offset, gain, penalty_init, samples, targets.T, member[None, :], omega,
        phase[None, :], factors, weights_init.T, duals_init.T, consensus_init.T,
    )
    return (final[0].T, final[1].T, final[2].T, history[:, :ITERS])


def solution(mesh):
    sizes = (mesh.shape["region"], mesh.shape["feat"], mesh.shape["row"])
    return jax.shard_map(
        functools.partial(per_device, sizes),
        mesh=mesh,
        in_specs=(
            P(("region", "row"), None),
            P(("region", "row"), None),
            P(("region", "row")),
            P(None, "feat"),
            P("feat"),
            P(("region", "feat"), None),
            P(("region", "feat"), "row"),
            P(("region", "feat"), "row"),
            P("feat", "row"),
            P("region"),
        ),
        out_specs=(
            P(("region", "feat"), "row"),
            P(("region", "feat"), "row"),
            P("feat", "row"),
            P("region", None),
        ),
        check_vma=False,
    )
```

```python
import functools
import math

import jax
import jax.numpy as jnp
from jax import lax
from jax.experimental import pallas as pl
from jax.experimental.pallas import tpu as pltpu
from jax.sharding import PartitionSpec as P

ITERS = 3
CORES = 2
PARTS = 2
MESH = pl.DeviceIdType.MESH
INV_TURN = 1.0 / (2.0 * math.pi)
SINE_TERMS = (6.1875, -40.5, 72.5)
SINE_GAIN = 1.0153050682891251
F32 = jnp.float32
BF16 = jnp.bfloat16


def dot(a, b):
    return lax.dot_general(a, b, (((1,), (0,)), ((), ())), preferred_element_type=F32)


def dot_nt(a, b):
    return lax.dot_general(a, b, (((1,), (1,)), ((), ())), preferred_element_type=F32)


def feature_tile(turns):
    rest = turns - jnp.round(turns)
    wave = (0.25 - jnp.abs(rest)).astype(BF16)
    square = wave * wave
    value = jnp.bfloat16(SINE_TERMS[-1])
    for term in SINE_TERMS[-2::-1]:
        value = value * square + jnp.bfloat16(term)
    return wave * value


def normalise(base, factor_ref, dinv_ref, n_ref):
    size = factor_ref.shape[0]
    for start in range(0, size, base):
        rows = factor_ref[start : start + base, :]
        row = lax.broadcasted_iota(jnp.int32, rows.shape, 0) + start
        column = lax.broadcasted_iota(jnp.int32, rows.shape, 1)
        diagonal = jnp.sum(jnp.where(row == column, rows, 0.0), axis=1, keepdims=True)
        n_ref[start : start + base, :] = jnp.where(row > column, rows / diagonal, 0.0).astype(BF16)
        block = factor_ref[start : start + base, start : start + base]
        inner_row = lax.broadcasted_iota(jnp.int32, block.shape, 0)
        inner_column = lax.broadcasted_iota(jnp.int32, block.shape, 1)
        on = jnp.sum(jnp.where(inner_row == inner_column, block, 0.0), axis=0, keepdims=True)
        dinv_ref[:, start : start + base] = 1.0 / on


def invert(base, n_ref, t_ref):
    size = n_ref.shape[0]
    t_ref[...] = jnp.zeros_like(t_ref)
    powers, totals = [], []
    for start in range(0, size, base):
        power = -n_ref[start : start + base, start : start + base].astype(F32)
        powers.append(power)
        totals.append(power)
    reach = 2
    while reach < base:
        for index in range(len(powers)):
            low = powers[index].astype(BF16)
            square = dot(low, low)
            low = square.astype(BF16)
            totals[index] = totals[index] + square + dot(totals[index].astype(BF16), low)
            powers[index] = square
        reach *= 2
    for index, start in enumerate(range(0, size, base)):
        t_ref[start : start + base, start : start + base] = totals[index].astype(BF16)
    width = base
    while width < size:
        for start in range(0, size, 2 * width):
            top = slice(start, start + width)
            bottom = slice(start + width, start + 2 * width)
            below = n_ref[bottom, top]
            first = below.astype(F32) + dot(below, t_ref[top, top])
            second = first + dot(t_ref[bottom, bottom], first.astype(BF16))
            t_ref[bottom, top] = (-second).astype(BF16)
        width *= 2


def admm_kernel(
    sizes,
    offset,
    gain,
    penalty_ref,
    samples_hbm,
    targets_hbm,
    member_hbm,
    omega_hbm,
    phase_hbm,
    factor_hbm,
    weights_hbm,
    duals_hbm,
    consensus_hbm,
    out_ref,
    history_ref,
    omega_ref,
    phase_ref,
    state_ref,
    factor_ref,
    dinv_ref,
    strict_ref,
    solve_ref,
    samples_ref,
    targets_ref,
    member_ref,
    far_omega_ref,
    far_phase_ref,
    wave_ref,
    twin_ref,
    feat_ref,
    across_ref,
    coarse_ref,
    acc_ref,
    part_ref,
    other_ref,
    resid_ref,
    total_ref,
    gfar_ref,
    gside_ref,
    gsum_ref,
    gsend_ref,
    grow_ref,
    reg_ref,
    gap_ref,
    load_sem,
    omega_send,
    omega_recv,
    crow_send,
    crow_recv,
    cside_send,
    cside_recv,
    core_send,
    core_recv,
    gside_send,
    gside_recv,
    grow_send,
    grow_recv,
    reg_send,
    reg_recv,
    gap_send,
    gap_recv,
):
    n_region, n_feat, n_row = sizes
    narrow, width = weights_hbm.shape
    outputs = n_row * narrow
    count = feat_ref.shape[2]
    chunk = min(2048, count)
    chunks = count // chunk
    piece_width = width // PARTS
    tile, base = min(512, width), min(256, width)
    inputs = samples_ref.shape[1]
    region, feat, row = lax.axis_index("region"), lax.axis_index("feat"), lax.axis_index("row")
    outward = sorted(range(1, n_row), key=lambda k: -min(k, n_row - k))
    inward = outward[::-1]
    group = n_feat * n_row
    place = feat * n_row + row
    across_feat = lax.rem(feat + CORES, n_feat)
    side_feat = across_feat + 1 - 2 * lax.rem(across_feat, CORES)
    side = (region, side_feat, row)
    core = (region, feat + 1 - 2 * lax.rem(feat, CORES), row)

    def row_peer(k):
        return (region, feat, lax.rem(row + k, n_row))

    def side_peer(k):
        return (region, side_feat, lax.rem(row + k, n_row))

    def region_peer(k):
        return (lax.rem(region + k, n_region), feat, row)

    def group_peer(k):
        other = lax.rem(place + k, group)
        return (region, other // n_row, lax.rem(other, n_row))

    def remote(src, dst, send, recv, device):
        return pltpu.make_async_remote_copy(
            src_ref=src, dst_ref=dst, send_sem=send, recv_sem=recv,
            device_id=device, device_id_type=MESH,
        )

    first = pl.multiple_of((feat // CORES) * count, 128)
    span = pl.ds(first, count)
    loads = [
        pltpu.make_async_copy(samples_hbm.at[span], samples_ref, load_sem.at[0]),
        pltpu.make_async_copy(targets_hbm.at[:, span], targets_ref, load_sem.at[1]),
        pltpu.make_async_copy(member_hbm.at[:, span], member_ref, load_sem.at[2]),
        pltpu.make_async_copy(factor_hbm, factor_ref, load_sem.at[3]),
        pltpu.make_async_copy(omega_hbm, omega_ref, load_sem.at[4]),
        pltpu.make_async_copy(phase_hbm, phase_ref, load_sem.at[5]),
        pltpu.make_async_copy(weights_hbm, state_ref.at[0], load_sem.at[6]),
        pltpu.make_async_copy(duals_hbm, state_ref.at[1], load_sem.at[7]),
        pltpu.make_async_copy(consensus_hbm, state_ref.at[2], load_sem.at[8]),
    ]
    for index in (4, 5, 0, 6, 7, 8, 1, 2, 3):
        loads[index].start()

    barrier = pltpu.get_barrier_semaphore()
    for k in range(1, group):
        pl.semaphore_signal(barrier, inc=1, device_id=group_peer(k), device_id_type=MESH)
    for k in range(1, n_region):
        pl.semaphore_signal(barrier, inc=1, device_id=region_peer(k), device_id_type=MESH)

    def prepare(half, omega, phase):
        exact = omega.astype(F32) * INV_TURN
        high = exact.astype(BF16)
        low = exact - high.astype(F32)
        turn = phase * INV_TURN
        first = turn.astype(BF16).astype(F32)
        level = lax.broadcasted_iota(jnp.int32, low.shape, 0)
        low = jnp.where(level == inputs - 2, first, jnp.where(level == inputs - 1, turn - first, low))
        wave_ref[half, :, :inputs] = high.T
        wave_ref[half, :, inputs:] = low.astype(BF16).T

    def fill(half):
        def step(i, carry):
            down = pl.multiple_of(i * tile, tile)
            value = feature_tile(dot_nt(wave_ref[half, pl.ds(down, tile), :], twin_ref[...]))
            feat_ref[half, pl.ds(down, tile), :] = value
            across_ref[half, :, pl.ds(down, tile)] = value.T
            return carry

        lax.fori_loop(0, width // tile, step, 0)

    rho = jnp.full((1, 128), penalty_ref[0], F32)
    history = jnp.zeros((1, 128), F32)
    lane = lax.broadcasted_iota(jnp.int32, (1, 128), 1)
    loads[4].wait()
    loads[5].wait()
    pl.semaphore_wait(barrier, group - 1 + n_region - 1)
    sends = []
    exchange = [
        remote(omega_ref, far_omega_ref, omega_send.at[0], omega_recv.at[0], side),
        remote(phase_ref, far_phase_ref, omega_send.at[1], omega_recv.at[1], side),
    ]
    for copy in exchange:
        copy.start()
        sends.append(copy)
    prepare(0, omega_ref[...], phase_ref[...])
    loads[0].wait()
    samples = samples_ref[...]
    place_in = lax.broadcasted_iota(jnp.int32, samples.shape, 1)
    twin_ref[:, :inputs] = samples
    twin_ref[:, inputs:] = jnp.where(place_in < inputs - 2, samples.astype(F32), 1.0).astype(BF16)
    for index in (6, 7, 8):
        loads[index].wait()
    weights, duals, consensus = state_ref[0], state_ref[1], state_ref[2]

    for t in range(ITERS):
        coarse_ref[t, 0, row] = weights.astype(BF16)
        mine = coarse_ref.at[t, 0, row]
        for k in outward:
            copy = remote(mine, mine, crow_send.at[t, k], crow_recv.at[t, k], row_peer(k))
            copy.start()
            sends.append(copy)
        if t == 0:
            fill(0)
        for k in outward + [0]:
            copy = remote(
                mine, coarse_ref.at[t, 1, row], cside_send.at[t, k], cside_recv.at[t, k],
                side_peer(k),
            )
            copy.start()
            sends.append(copy)

        for k in inward:
            source = lax.rem(row - k + n_row, n_row)
            piece = coarse_ref.at[t, 0, source]
            remote(piece, piece, crow_send.at[t, k], crow_recv.at[t, k], side).wait_recv()
        near = coarse_ref[t, 0].reshape(outputs, width)
        for j in range(chunks):
            span = slice(j * chunk, (j + 1) * chunk)
            acc_ref[:, span] = dot(near, feat_ref[0, :, span])
        if t == 0:
            for copy in exchange:
                copy.wait_recv()
            prepare(1, far_omega_ref[...], far_phase_ref[...])
            fill(1)
            loads[1].wait()
            loads[2].wait()
        for k in range(n_row):
            source = lax.rem(row - k + n_row, n_row)
            piece = coarse_ref.at[t, 1, source]
            remote(piece, piece, cside_send.at[t, k], cside_recv.at[t, k], side).wait_recv()
        far = coarse_ref[t, 1].reshape(outputs, width)
        for j in range(chunks):
            span = slice(j * chunk, (j + 1) * chunk)
            part = acc_ref[:, span] + dot(far, feat_ref[1, :, span])
            acc_ref[:, span] = part
            part_ref[t, j] = part.astype(BF16)
            copy = remote(
                part_ref.at[t, j], other_ref.at[t, j], core_send.at[t, j], core_recv.at[t, j], core
            )
            copy.start()
            sends.append(copy)
        if t > 0:
            duals, consensus = finish_region(t - 1)
        for j in range(chunks):
            span = slice(j * chunk, (j + 1) * chunk)
            piece = other_ref.at[t, j]
            remote(piece, piece, core_send.at[t, j], core_recv.at[t, j], core).wait_recv()
            predicted = gain * (acc_ref[:, span] + other_ref[t, j].astype(F32))
            gap_value = predicted - targets_ref[:, span].astype(F32)
            resid_ref[:, span] = (member_ref[:, span].astype(F32) * gap_value).astype(BF16)
            if j < chunks - 1:
                value = dot(resid_ref[:, span], across_ref[1, span, :])
                total_ref[...] = value if j == 0 else total_ref[...] + value

        last = slice((chunks - 1) * chunk, chunks * chunk)
        for p in range(PARTS):
            span = slice(p * piece_width, (p + 1) * piece_width)
            value = dot(resid_ref[:, last], across_ref[1, last, span])
            if chunks > 1:
                value = value + total_ref[:, span]
            gfar_ref[t, p] = value.astype(BF16).reshape(n_row, narrow, piece_width)
            for k in outward + [0]:
                target = lax.rem(row + k, n_row)
                copy = remote(
                    gfar_ref.at[t, p, target], gside_ref.at[t, p, k], gside_send.at[t, p, k],
                    gside_recv.at[t, p, k], side_peer(k),
                )
                copy.start()
                sends.append(copy)
        for p in range(PARTS):
            span = slice(p * piece_width, (p + 1) * piece_width)
            value = dot(resid_ref[...], across_ref[0, :, span])
            gsum_ref[p] = value.reshape(n_row, narrow, piece_width)
            gsend_ref[t, p] = value.astype(BF16).reshape(n_row, narrow, piece_width)
            for k in outward:
                target = lax.rem(row + k, n_row)
                copy = remote(
                    gsend_ref.at[t, p, target], grow_ref.at[t, p, k], grow_send.at[t, p, k],
                    grow_recv.at[t, p, k], row_peer(k),
                )
                copy.start()
                sends.append(copy)
        if t == 0:
            loads[3].wait()
            normalise(base, factor_ref, dinv_ref, strict_ref)
        if t > 0:
            rho, duals, history = finish_gap(t - 1, rho, duals, history)
        else:
            invert(base, strict_ref, solve_ref)
        dinv = dinv_ref[...]
        scalar = rho[:, :1]
        gradient = []
        for p in range(PARTS):
            value = gsum_ref[p, row]
            for k in range(n_row):
                piece = gside_ref.at[t, p, k]
                remote(
                    piece, piece, gside_send.at[t, p, k], gside_recv.at[t, p, k], side
                ).wait_recv()
                value = value + gside_ref[t, p, k].astype(F32)
            for k in range(1, n_row):
                piece = grow_ref.at[t, p, k]
                remote(
                    piece, piece, grow_send.at[t, p, k], grow_recv.at[t, p, k], side
                ).wait_recv()
                value = value + grow_ref[t, p, k].astype(F32)
            gradient.append(value)
        right = scalar * (weights - consensus + duals) + gain * jnp.concatenate(gradient, axis=1)
        forward = right * dinv
        low = forward.astype(BF16)
        steps = [
            dot_nt(low[:, : start + base], solve_ref[start : start + base, : start + base])
            for start in range(0, width, base)
        ]
        forward = forward + jnp.concatenate(steps, axis=1)
        low = forward.astype(BF16)
        steps = [
            dot(low[:, start:], solve_ref[start:, start : start + base])
            for start in range(0, width, base)
        ]
        backward = (forward + jnp.concatenate(steps, axis=1)) * dinv
        weights = weights - backward

        reg_ref[t, region, :narrow] = scalar * (weights + duals)
        reg_ref[t, region, narrow:] = jnp.broadcast_to(scalar, (8, width))
        mine = reg_ref.at[t, region]
        for k in range(1, n_region):
            copy = remote(mine, mine, reg_send.at[t, k], reg_recv.at[t, k], region_peer(k))
            copy.start()
            sends.append(copy)

        def finish_region(s, weights=weights, duals=duals, consensus=consensus):
            for k in range(1, n_region):
                source = lax.rem(region - k + n_region, n_region)
                piece = reg_ref.at[s, source]
                remote(
                    piece, piece, reg_send.at[s, k], reg_recv.at[s, k], region_peer(k)
                ).wait_recv()
            total = reg_ref[s, 0]
            for r in range(1, n_region):
                total = total + reg_ref[s, r]
            updated = total[:narrow] / total[narrow : narrow + 1]
            gap = jnp.sum(jnp.square(weights - updated), keepdims=True).reshape(1, 1)
            drift = jnp.sum(jnp.square(updated - consensus), keepdims=True).reshape(1, 1)
            level = lax.broadcasted_iota(jnp.int32, (8, 128), 0)
            gap_ref[s, place] = jnp.where(level == 0, gap, drift)
            mine = gap_ref.at[s, place]
            for k in range(1, group):
                copy = remote(mine, mine, gap_send.at[s, k], gap_recv.at[s, k], group_peer(k))
                copy.start()
                sends.append(copy)
            return duals + weights - updated, updated

        def finish_gap(s, rho, duals, history):
            for k in range(1, group):
                source = lax.rem(place - k + group, group)
                piece = gap_ref.at[s, source]
                remote(
                    piece, piece, gap_send.at[s, k], gap_recv.at[s, k], group_peer(k)
                ).wait_recv()
            total = jnp.sum(gap_ref[s], axis=0)
            gap, drift = total[0:1], total[1:2]
            drift = rho * rho * drift
            renewed = rho * jnp.sqrt((gap + offset) / (drift + offset))
            duals = duals * (rho / renewed)[:, :1]
            return renewed, duals, jnp.where(lane == s, renewed, history)

    duals, consensus = finish_region(ITERS - 1)
    rho, duals, history = finish_gap(ITERS - 1, rho, duals, history)
    out_ref[0] = weights
    out_ref[1] = duals
    out_ref[2] = consensus
    history_ref[...] = history
    for copy in sends:
        copy.wait_send()


def admm(sizes, offset, gain, penalty, samples, targets, member, omega, phase, factors, *state):
    n_region, n_feat, n_row = sizes
    narrow, width = state[0].shape
    outputs = n_row * narrow
    inputs = omega.shape[0]
    count = samples.shape[0] // (n_feat // CORES)
    chunk = min(2048, count)
    chunks = count // chunk
    group = n_feat * n_row
    part = (n_row, narrow, width // PARTS)
    vmem = pl.BlockSpec(memory_space=pltpu.VMEM)
    hbm = pl.BlockSpec(memory_space=pl.ANY)
    dma = pltpu.SemaphoreType.DMA
    return pl.pallas_call(
        functools.partial(admm_kernel, sizes, offset, gain),
        in_specs=[pl.BlockSpec(memory_space=pltpu.SMEM), ] + [hbm] * 9,
        out_specs=[vmem, vmem],
        out_shape=[
            pltpu.VMEM((3, narrow, width), F32),
            pltpu.VMEM((1, 128), F32),
        ],
        scratch_shapes=[
            pltpu.VMEM((inputs, width), BF16),
            pltpu.VMEM((1, width), F32),
            pltpu.VMEM((3, narrow, width), F32),
            pltpu.VMEM((width, width), F32),
            pltpu.VMEM((1, width), F32),
            pltpu.VMEM((width, width), BF16),
            pltpu.VMEM((width, width), BF16),
            pltpu.VMEM((count, inputs), BF16),
            pltpu.VMEM((outputs, count), BF16),
            pltpu.VMEM((1, count), jnp.int32),
            pltpu.VMEM((inputs, width), BF16),
            pltpu.VMEM((1, width), F32),
            pltpu.VMEM((2, width, 2 * inputs), BF16),
            pltpu.VMEM((count, 2 * inputs), BF16),
            pltpu.VMEM((2, width, count), BF16),
            pltpu.VMEM((2, count, width), BF16),
            pltpu.VMEM((ITERS, 2, n_row, narrow, width), BF16),
            pltpu.VMEM((outputs, count), F32),
            pltpu.VMEM((ITERS, chunks, outputs, chunk), BF16),
            pltpu.VMEM((ITERS, chunks, outputs, chunk), BF16),
            pltpu.VMEM((outputs, count), BF16),
            pltpu.VMEM((outputs, width), F32),
            pltpu.VMEM((ITERS, PARTS) + part, BF16),
            pltpu.VMEM((ITERS, PARTS) + part, BF16),
            pltpu.VMEM((PARTS,) + part, F32),
            pltpu.VMEM((ITERS, PARTS) + part, BF16),
            pltpu.VMEM((ITERS, PARTS) + part, BF16),
            pltpu.VMEM((ITERS, n_region, narrow + 8, width), F32),
            pltpu.VMEM((ITERS, group, 8, 128), F32),
            dma((9,)),
            dma((2,)),
            dma((2,)),
            dma((ITERS, n_row)),
            dma((ITERS, n_row)),
            dma((ITERS, n_row)),
            dma((ITERS, n_row)),
            dma((ITERS, chunks)),
            dma((ITERS, chunks)),
            dma((ITERS, PARTS, n_row)),
            dma((ITERS, PARTS, n_row)),
            dma((ITERS, PARTS, n_row)),
            dma((ITERS, PARTS, n_row)),
            dma((ITERS, n_region)),
            dma((ITERS, n_region)),
            dma((ITERS, group)),
            dma((ITERS, group)),
        ],
        compiler_params=pltpu.CompilerParams(
            collective_id=0, has_side_effects=True, vmem_limit_bytes=60 * 2**20
        ),
        name="admm",
    )(penalty, samples, targets, member, omega, phase, factors, *state)


def per_device(
    sizes,
    samples,
    targets,
    member,
    omega,
    phase,
    factors,
    weights_init,
    duals_init,
    consensus_init,
    penalty_init,
):
    n_region, n_feat, n_row = sizes
    total_features = n_feat * omega.shape[1]
    total_outputs = targets.shape[1]
    offset = 0.01 * total_features * total_outputs
    gain = SINE_GAIN * math.sqrt(2.0 / total_features)
    final, history = admm(
        sizes, offset, gain, penalty_init, samples, targets.T, member[None, :], omega,
        phase[None, :], factors, weights_init.T, duals_init.T, consensus_init.T,
    )
    return (final[0].T, final[1].T, final[2].T, history[:, :ITERS])


def solution(mesh):
    sizes = (mesh.shape["region"], mesh.shape["feat"], mesh.shape["row"])
    return jax.shard_map(
        functools.partial(per_device, sizes),
        mesh=mesh,
        in_specs=(
            P(("region", "row"), None),
            P(("region", "row"), None),
            P(("region", "row")),
            P(None, "feat"),
            P("feat"),
            P(("region", "feat"), None),
            P(("region", "feat"), "row"),
            P(("region", "feat"), "row"),
            P("feat", "row"),
            P("region"),
        ),
        out_specs=(
            P(("region", "feat"), "row"),
            P(("region", "feat"), "row"),
            P("feat", "row"),
            P("region", None),
        ),
        check_vma=False,
    )
```

```python
import functools
import math

import jax
import jax.numpy as jnp
from jax import lax
from jax.experimental import pallas as pl
from jax.experimental.pallas import tpu as pltpu
from jax.sharding import PartitionSpec as P

ITERS = 3
CORES = 2
PARTS = 2
MESH = pl.DeviceIdType.MESH
INV_TURN = 1.0 / (2.0 * math.pi)
SINE_TERMS = (6.1875, -40.5, 72.5)
SINE_GAIN = 1.0153050682891251
F32 = jnp.float32
BF16 = jnp.bfloat16


def dot(a, b):
    return lax.dot_general(a, b, (((1,), (0,)), ((), ())), preferred_element_type=F32)


def dot_nt(a, b):
    return lax.dot_general(a, b, (((1,), (1,)), ((), ())), preferred_element_type=F32)


def feature_tile(turns):
    rest = turns - jnp.round(turns)
    wave = (0.25 - jnp.abs(rest)).astype(BF16)
    square = wave * wave
    value = jnp.bfloat16(SINE_TERMS[-1])
    for term in SINE_TERMS[-2::-1]:
        value = value * square + jnp.bfloat16(term)
    return wave * value


def normalise(base, factor_ref, dinv_ref, n_ref):
    size = factor_ref.shape[0]
    for start in range(0, size, base):
        rows = factor_ref[start : start + base, :]
        row = lax.broadcasted_iota(jnp.int32, rows.shape, 0) + start
        column = lax.broadcasted_iota(jnp.int32, rows.shape, 1)
        diagonal = jnp.sum(jnp.where(row == column, rows, 0.0), axis=1, keepdims=True)
        n_ref[start : start + base, :] = jnp.where(row > column, rows / diagonal, 0.0).astype(BF16)
        block = factor_ref[start : start + base, start : start + base]
        inner_row = lax.broadcasted_iota(jnp.int32, block.shape, 0)
        inner_column = lax.broadcasted_iota(jnp.int32, block.shape, 1)
        on = jnp.sum(jnp.where(inner_row == inner_column, block, 0.0), axis=0, keepdims=True)
        dinv_ref[:, start : start + base] = 1.0 / on


def invert(base, n_ref, t_ref):
    size = n_ref.shape[0]
    t_ref[...] = jnp.zeros_like(t_ref)
    powers, totals = [], []
    for start in range(0, size, base):
        power = -n_ref[start : start + base, start : start + base].astype(F32)
        powers.append(power)
        totals.append(power)
    reach = 2
    while reach < base:
        for index in range(len(powers)):
            low = powers[index].astype(BF16)
            square = dot(low, low)
            low = square.astype(BF16)
            totals[index] = totals[index] + square + dot(totals[index].astype(BF16), low)
            powers[index] = square
        reach *= 2
    for index, start in enumerate(range(0, size, base)):
        t_ref[start : start + base, start : start + base] = totals[index].astype(BF16)
    width = base
    while width < size:
        for start in range(0, size, 2 * width):
            top = slice(start, start + width)
            bottom = slice(start + width, start + 2 * width)
            below = n_ref[bottom, top]
            first = below.astype(F32) + dot(below, t_ref[top, top])
            second = first + dot(t_ref[bottom, bottom], first.astype(BF16))
            t_ref[bottom, top] = (-second).astype(BF16)
        width *= 2


def admm_kernel(
    sizes,
    offset,
    gain,
    penalty_hbm,
    samples_hbm,
    targets_hbm,
    member_hbm,
    omega_hbm,
    phase_hbm,
    factor_hbm,
    weights_hbm,
    duals_hbm,
    consensus_hbm,
    out_ref,
    history_ref,
    penalty_ref,
    omega_ref,
    phase_ref,
    state_ref,
    factor_ref,
    dinv_ref,
    strict_ref,
    solve_ref,
    samples_ref,
    targets_ref,
    member_ref,
    far_omega_ref,
    far_phase_ref,
    wave_ref,
    twin_ref,
    feat_ref,
    across_ref,
    coarse_ref,
    acc_ref,
    part_ref,
    other_ref,
    resid_ref,
    total_ref,
    gfar_ref,
    gside_ref,
    gsum_ref,
    gsend_ref,
    grow_ref,
    reg_ref,
    rate_ref,
    gap_ref,
    load_sem,
    omega_send,
    omega_recv,
    crow_send,
    crow_recv,
    cside_send,
    cside_recv,
    core_send,
    core_recv,
    gside_send,
    gside_recv,
    grow_send,
    grow_recv,
    reg_send,
    reg_recv,
    gap_send,
    gap_recv,
):
    n_region, n_feat, n_row = sizes
    narrow, width = weights_hbm.shape
    outputs = n_row * narrow
    count = feat_ref.shape[2]
    chunk = min(2048, count)
    chunks = count // chunk
    piece_width = width // PARTS
    tile, base = min(512, width), min(256, width)
    inputs = samples_ref.shape[1]
    region, feat, row = lax.axis_index("region"), lax.axis_index("feat"), lax.axis_index("row")
    outward = sorted(range(1, n_row), key=lambda k: -min(k, n_row - k))
    inward = outward[::-1]
    ties = [k for k in outward if 2 * k == n_row]
    direct = [k for k in outward if 2 * k != n_row]
    group = n_feat * n_row
    place = feat * n_row + row
    across_feat = lax.rem(feat + CORES, n_feat)
    side_feat = across_feat + 1 - 2 * lax.rem(across_feat, CORES)
    side = (region, side_feat, row)
    core = (region, feat + 1 - 2 * lax.rem(feat, CORES), row)

    def row_peer(k):
        return (region, feat, lax.rem(row + k, n_row))

    def side_peer(k):
        return (region, side_feat, lax.rem(row + k, n_row))

    def region_peer(k):
        return (lax.rem(region + k, n_region), feat, row)

    def group_peer(k):
        other = lax.rem(place + k, group)
        return (region, other // n_row, lax.rem(other, n_row))

    def remote(src, dst, send, recv, device):
        return pltpu.make_async_remote_copy(
            src_ref=src, dst_ref=dst, send_sem=send, recv_sem=recv,
            device_id=device, device_id_type=MESH,
        )

    first = pl.multiple_of((feat // CORES) * count, 128)
    span = pl.ds(first, count)
    loads = [
        pltpu.make_async_copy(samples_hbm.at[span], samples_ref, load_sem.at[0]),
        pltpu.make_async_copy(targets_hbm.at[:, span], targets_ref, load_sem.at[1]),
        pltpu.make_async_copy(member_hbm.at[:, span], member_ref, load_sem.at[2]),
        pltpu.make_async_copy(factor_hbm, factor_ref, load_sem.at[3]),
        pltpu.make_async_copy(omega_hbm, omega_ref, load_sem.at[4]),
        pltpu.make_async_copy(phase_hbm, phase_ref, load_sem.at[5]),
        pltpu.make_async_copy(weights_hbm, state_ref.at[0], load_sem.at[6]),
        pltpu.make_async_copy(duals_hbm, state_ref.at[1], load_sem.at[7]),
        pltpu.make_async_copy(consensus_hbm, state_ref.at[2], load_sem.at[8]),
        pltpu.make_async_copy(penalty_hbm, penalty_ref, load_sem.at[9]),
    ]
    for index in (4, 5, 0, 6, 7, 8, 9, 1, 2, 3):
        loads[index].start()

    barrier = pltpu.get_barrier_semaphore()
    for k in range(1, group):
        pl.semaphore_signal(barrier, inc=1, device_id=group_peer(k), device_id_type=MESH)
    for k in range(1, n_region):
        pl.semaphore_signal(barrier, inc=1, device_id=region_peer(k), device_id_type=MESH)

    def prepare(half, down, omega, phase):
        exact = omega.astype(F32) * INV_TURN
        high = exact.astype(BF16)
        low = exact - high.astype(F32)
        turn = phase * INV_TURN
        first = turn.astype(BF16).astype(F32)
        level = lax.broadcasted_iota(jnp.int32, low.shape, 0)
        low = jnp.where(level == inputs - 2, first, jnp.where(level == inputs - 1, turn - first, low))
        wave_ref[half, down, :inputs] = high.T
        wave_ref[half, down, inputs:] = low.astype(BF16).T

    tiles = [slice(start, start + tile) for start in range(0, width, tile)]

    def fill(half, down):
        value = feature_tile(dot_nt(wave_ref[half, down, :], twin_ref[...]))
        feat_ref[half, down, :] = value
        across_ref[half, :, down] = value.T

    history = jnp.zeros((1, 128), F32)
    lane = lax.broadcasted_iota(jnp.int32, (1, 128), 1)
    loads[4].wait()
    loads[5].wait()
    pl.semaphore_wait(barrier, group - 1 + n_region - 1)
    sends = []
    exchange = [remote(phase_ref, far_phase_ref, omega_send.at[0], omega_recv.at[0], side)]
    for i, down in enumerate(tiles):
        exchange.append(
            remote(
                omega_ref.at[:, down], far_omega_ref.at[:, down], omega_send.at[i + 1],
                omega_recv.at[i + 1], side,
            )
        )
    for copy in exchange:
        copy.start()
        sends.append(copy)
    prepare(0, slice(0, width), omega_ref[...], phase_ref[...])
    loads[0].wait()
    samples = samples_ref[...]
    place_in = lax.broadcasted_iota(jnp.int32, samples.shape, 1)
    twin_ref[:, :inputs] = samples
    twin_ref[:, inputs:] = jnp.where(place_in < inputs - 2, samples.astype(F32), 1.0).astype(BF16)
    for index in (6, 7, 8, 9):
        loads[index].wait()
    rho = jnp.full((1, 128), penalty_ref[0], F32)
    weights, duals, consensus = state_ref[0], state_ref[1], state_ref[2]

    for t in range(ITERS):
        coarse_ref[t, 0, row] = weights.astype(BF16)
        mine = coarse_ref.at[t, 0, row]
        for k in outward:
            copy = remote(mine, mine, crow_send.at[t, k], crow_recv.at[t, k], row_peer(k))
            copy.start()
            sends.append(copy)
        if t == 0:
            for down in tiles:
                fill(0, down)
        for k in direct + [0]:
            copy = remote(
                mine, coarse_ref.at[t, 1, row], cside_send.at[t, k], cside_recv.at[t, k],
                side_peer(k),
            )
            copy.start()
            sends.append(copy)

        for k in inward:
            source = lax.rem(row - k + n_row, n_row)
            piece = coarse_ref.at[t, 0, source]
            remote(piece, piece, crow_send.at[t, k], crow_recv.at[t, k], side).wait_recv()
            if k in ties:
                copy = remote(
                    piece, coarse_ref.at[t, 1, source], cside_send.at[t, k], cside_recv.at[t, k],
                    side,
                )
                copy.start()
                sends.append(copy)
        near = coarse_ref[t, 0].reshape(outputs, width)
        if t > 0:
            for j in range(chunks):
                span = slice(j * chunk, (j + 1) * chunk)
                acc_ref[:, span] = dot(near, feat_ref[0, :, span])
        else:
            stretch = count // len(tiles)
            exchange[0].wait_recv()
            for i, down in enumerate(tiles):
                exchange[i + 1].wait_recv()
                prepare(1, down, far_omega_ref[:, down], far_phase_ref[:, down])
                fill(1, down)
                span = slice(i * stretch, (i + 1) * stretch)
                acc_ref[:, span] = dot(near, feat_ref[0, :, span])
            loads[1].wait()
            loads[2].wait()
        for k in range(n_row):
            source = lax.rem(row - k + n_row, n_row)
            piece = coarse_ref.at[t, 1, source]
            remote(piece, piece, cside_send.at[t, k], cside_recv.at[t, k], side).wait_recv()
        far = coarse_ref[t, 1].reshape(outputs, width)
        for j in range(chunks):
            span = slice(j * chunk, (j + 1) * chunk)
            part = acc_ref[:, span] + dot(far, feat_ref[1, :, span])
            acc_ref[:, span] = part
            part_ref[t, j] = part.astype(BF16)
            copy = remote(
                part_ref.at[t, j], other_ref.at[t, j], core_send.at[t, j], core_recv.at[t, j], core
            )
            copy.start()
            sends.append(copy)
        if t > 0:
            duals, consensus = finish_region(t - 1)
        for j in range(chunks):
            span = slice(j * chunk, (j + 1) * chunk)
            piece = other_ref.at[t, j]
            remote(piece, piece, core_send.at[t, j], core_recv.at[t, j], core).wait_recv()
            predicted = gain * (acc_ref[:, span] + other_ref[t, j].astype(F32))
            gap_value = predicted - targets_ref[:, span].astype(F32)
            resid_ref[:, span] = (member_ref[:, span].astype(F32) * gap_value).astype(BF16)
            if j < chunks - 1:
                value = dot(resid_ref[:, span], across_ref[1, span, :])
                total_ref[...] = value if j == 0 else total_ref[...] + value

        last = slice((chunks - 1) * chunk, chunks * chunk)
        for p in range(PARTS):
            span = slice(p * piece_width, (p + 1) * piece_width)
            value = dot(resid_ref[:, last], across_ref[1, last, span])
            if chunks > 1:
                value = value + total_ref[:, span]
            gfar_ref[t, p] = value.astype(BF16).reshape(n_row, narrow, piece_width)
            for k in outward + [0]:
                target = lax.rem(row + k, n_row)
                copy = remote(
                    gfar_ref.at[t, p, target], gside_ref.at[t, p, k], gside_send.at[t, p, k],
                    gside_recv.at[t, p, k], side_peer(k),
                )
                copy.start()
                sends.append(copy)
        for p in range(PARTS):
            span = slice(p * piece_width, (p + 1) * piece_width)
            value = dot(resid_ref[...], across_ref[0, :, span])
            gsum_ref[p] = value.reshape(n_row, narrow, piece_width)
            gsend_ref[t, p] = value.astype(BF16).reshape(n_row, narrow, piece_width)
            for k in outward:
                target = lax.rem(row + k, n_row)
                copy = remote(
                    gsend_ref.at[t, p, target], grow_ref.at[t, p, k], grow_send.at[t, p, k],
                    grow_recv.at[t, p, k], row_peer(k),
                )
                copy.start()
                sends.append(copy)
        if t == 0:
            loads[3].wait()
            normalise(base, factor_ref, dinv_ref, strict_ref)
        if t > 0:
            rho, duals, history = finish_gap(t - 1, rho, duals, history)
        else:
            invert(base, strict_ref, solve_ref)
        dinv = dinv_ref[...]
        scalar = rho[:, :1]
        gradient = []
        for p in range(PARTS):
            value = gsum_ref[p, row]
            for k in range(n_row):
                piece = gside_ref.at[t, p, k]
                remote(
                    piece, piece, gside_send.at[t, p, k], gside_recv.at[t, p, k], side
                ).wait_recv()
                value = value + gside_ref[t, p, k].astype(F32)
            for k in range(1, n_row):
                piece = grow_ref.at[t, p, k]
                remote(
                    piece, piece, grow_send.at[t, p, k], grow_recv.at[t, p, k], side
                ).wait_recv()
                value = value + grow_ref[t, p, k].astype(F32)
            gradient.append(value)
        right = scalar * (weights - consensus + duals) + gain * jnp.concatenate(gradient, axis=1)
        forward = right * dinv
        low = forward.astype(BF16)
        steps = [
            dot_nt(low[:, : start + base], solve_ref[start : start + base, : start + base])
            for start in range(0, width, base)
        ]
        forward = forward + jnp.concatenate(steps, axis=1)
        low = forward.astype(BF16)
        steps = [
            dot(low[:, start:], solve_ref[start:, start : start + base])
            for start in range(0, width, base)
        ]
        backward = (forward + jnp.concatenate(steps, axis=1)) * dinv
        weights = weights - backward

        reg_ref[t, region] = scalar * (weights + duals)
        rate_ref[t, region] = rho
        for part, ref in enumerate((reg_ref, rate_ref)):
            mine = ref.at[t, region]
            for k in range(1, n_region):
                copy = remote(
                    mine, mine, reg_send.at[t, part, k], reg_recv.at[t, part, k], region_peer(k)
                )
                copy.start()
                sends.append(copy)

        def finish_region(s, weights=weights, duals=duals, consensus=consensus):
            for part, ref in enumerate((reg_ref, rate_ref)):
                for k in range(1, n_region):
                    source = lax.rem(region - k + n_region, n_region)
                    piece = ref.at[s, source]
                    remote(
                        piece, piece, reg_send.at[s, part, k], reg_recv.at[s, part, k],
                        region_peer(k),
                    ).wait_recv()
            total, rate = reg_ref[s, 0], rate_ref[s, 0]
            for r in range(1, n_region):
                total, rate = total + reg_ref[s, r], rate + rate_ref[s, r]
            updated = total / rate[:, :1]
            gap = jnp.sum(jnp.square(weights - updated), keepdims=True).reshape(1, 1)
            drift = jnp.sum(jnp.square(updated - consensus), keepdims=True).reshape(1, 1)
            level = lax.broadcasted_iota(jnp.int32, (2, 128), 0)
            gap_ref[s, place] = jnp.where(level == 0, gap, drift)
            mine = gap_ref.at[s, place]
            for k in range(1, group):
                copy = remote(mine, mine, gap_send.at[s, k], gap_recv.at[s, k], group_peer(k))
                copy.start()
                sends.append(copy)
            return duals + weights - updated, updated

        def finish_gap(s, rho, duals, history):
            for k in range(1, group):
                source = lax.rem(place - k + group, group)
                piece = gap_ref.at[s, source]
                remote(
                    piece, piece, gap_send.at[s, k], gap_recv.at[s, k], group_peer(k)
                ).wait_recv()
            total = jnp.sum(gap_ref[s], axis=0)
            gap, drift = total[0:1], total[1:2]
            drift = rho * rho * drift
            renewed = rho * jnp.sqrt((gap + offset) / (drift + offset))
            duals = duals * (rho / renewed)[:, :1]
            return renewed, duals, jnp.where(lane == s, renewed, history)

    duals, consensus = finish_region(ITERS - 1)
    rho, duals, history = finish_gap(ITERS - 1, rho, duals, history)
    out_ref[0] = weights
    out_ref[1] = duals
    out_ref[2] = consensus
    history_ref[...] = history
    for copy in sends:
        copy.wait_send()


def admm(sizes, offset, gain, penalty, samples, targets, member, omega, phase, factors, *state):
    n_region, n_feat, n_row = sizes
    narrow, width = state[0].shape
    outputs = n_row * narrow
    inputs = omega.shape[0]
    count = samples.shape[0] // (n_feat // CORES)
    chunk = min(2048, count)
    chunks = count // chunk
    group = n_feat * n_row
    part = (n_row, narrow, width // PARTS)
    vmem = pl.BlockSpec(memory_space=pltpu.VMEM)
    hbm = pl.BlockSpec(memory_space=pl.ANY)
    dma = pltpu.SemaphoreType.DMA
    return pl.pallas_call(
        functools.partial(admm_kernel, sizes, offset, gain),
        in_specs=[hbm] * 10,
        out_specs=[vmem, vmem],
        out_shape=[
            pltpu.VMEM((3, narrow, width), F32),
            pltpu.VMEM((1, 128), F32),
        ],
        scratch_shapes=[
            pltpu.SMEM((1,), F32),
            pltpu.VMEM((inputs, width), BF16),
            pltpu.VMEM((1, width), F32),
            pltpu.VMEM((3, narrow, width), F32),
            pltpu.VMEM((width, width), F32),
            pltpu.VMEM((1, width), F32),
            pltpu.VMEM((width, width), BF16),
            pltpu.VMEM((width, width), BF16),
            pltpu.VMEM((count, inputs), BF16),
            pltpu.VMEM((outputs, count), BF16),
            pltpu.VMEM((1, count), jnp.int32),
            pltpu.VMEM((inputs, width), BF16),
            pltpu.VMEM((1, width), F32),
            pltpu.VMEM((2, width, 2 * inputs), BF16),
            pltpu.VMEM((count, 2 * inputs), BF16),
            pltpu.VMEM((2, width, count), BF16),
            pltpu.VMEM((2, count, width), BF16),
            pltpu.VMEM((ITERS, 2, n_row, narrow, width), BF16),
            pltpu.VMEM((outputs, count), F32),
            pltpu.VMEM((ITERS, chunks, outputs, chunk), BF16),
            pltpu.VMEM((ITERS, chunks, outputs, chunk), BF16),
            pltpu.VMEM((outputs, count), BF16),
            pltpu.VMEM((outputs, width), F32),
            pltpu.VMEM((ITERS, PARTS) + part, BF16),
            pltpu.VMEM((ITERS, PARTS) + part, BF16),
            pltpu.VMEM((PARTS,) + part, F32),
            pltpu.VMEM((ITERS, PARTS) + part, BF16),
            pltpu.VMEM((ITERS, PARTS) + part, BF16),
            pltpu.VMEM((ITERS, n_region, narrow, width), F32),
            pltpu.VMEM((ITERS, n_region, 1, 128), F32),
            pltpu.VMEM((ITERS, group, 2, 128), F32),
            dma((10,)),
            dma((1 + width // min(512, width),)),
            dma((1 + width // min(512, width),)),
            dma((ITERS, n_row)),
            dma((ITERS, n_row)),
            dma((ITERS, n_row)),
            dma((ITERS, n_row)),
            dma((ITERS, chunks)),
            dma((ITERS, chunks)),
            dma((ITERS, PARTS, n_row)),
            dma((ITERS, PARTS, n_row)),
            dma((ITERS, PARTS, n_row)),
            dma((ITERS, PARTS, n_row)),
            dma((ITERS, 2, n_region)),
            dma((ITERS, 2, n_region)),
            dma((ITERS, group)),
            dma((ITERS, group)),
        ],
        compiler_params=pltpu.CompilerParams(
            collective_id=0, has_side_effects=True, vmem_limit_bytes=60 * 2**20
        ),
        name="admm",
    )(penalty, samples, targets, member, omega, phase, factors, *state)


def per_device(
    sizes,
    samples,
    targets,
    member,
    omega,
    phase,
    factors,
    weights_init,
    duals_init,
    consensus_init,
    penalty_init,
):
    n_region, n_feat, n_row = sizes
    total_features = n_feat * omega.shape[1]
    total_outputs = targets.shape[1]
    offset = 0.01 * total_features * total_outputs
    gain = SINE_GAIN * math.sqrt(2.0 / total_features)
    final, history = admm(
        sizes, offset, gain, penalty_init, samples, targets.T, member[None, :], omega,
        phase[None, :], factors, weights_init.T, duals_init.T, consensus_init.T,
    )
    return (final[0].T, final[1].T, final[2].T, history[:, :ITERS])


def solution(mesh):
    sizes = (mesh.shape["region"], mesh.shape["feat"], mesh.shape["row"])
    return jax.shard_map(
        functools.partial(per_device, sizes),
        mesh=mesh,
        in_specs=(
            P(("region", "row"), None),
            P(("region", "row"), None),
            P(("region", "row")),
            P(None, "feat"),
            P("feat"),
            P(("region", "feat"), None),
            P(("region", "feat"), "row"),
            P(("region", "feat"), "row"),
            P("feat", "row"),
            P("region"),
        ),
        out_specs=(
            P(("region", "feat"), "row"),
            P(("region", "feat"), "row"),
            P("feat", "row"),
            P("region", None),
        ),
        check_vma=False,
    )
```
